32 devices in a mesh: dom: 32 (over z, y, x, core).
Axes of the slice: x: 2, y: 2, z: 4, core: 2. Of those that a mesh axis runs over, the one named last changes fastest.
Arguments:
- features: bfloat16 [16384, 512], P('dom'), may hold values from -6 to 6
- weights: bfloat16 [3, 512, 512], replicated, may hold values from -0.078125 to 0.078125
- halo_send: int32 [32, 32, 4], P('dom'), may hold values from 0 to 511
- nbr_index: int32 [16384, 2, 8], P('dom'), may hold values from 0 to 639
- tile_count: int32 [32], P('dom'), may hold values from 1 to 16, as said below
- edge_ends: int32 [512, 2, 256], P('dom'), may hold values from 0 to 511
- neg_ids: int32 [256], P('dom'), may hold values from 0 to 511
Outputs:
- weight_grad: float32 [3, 512, 512], replicated
- mean_loss: float32 [], replicated
- pre_grad: bfloat16 [16384, 512], P('dom')
The draws below stay inside these ranges and needn't reach their ends.
Inputs may be any that keep to these rules, and one draw needn't show every extreme that they name: `nbr_index`: an entry below 512 names a row of the node's own partition; an entry 512 + q * 4 + k names slot k of the halo from partition q. `tile_count`: partition 32 - 1 holds 16 tiles; every other partition holds at most 8. `edge_ends`: tile slots at or past a partition's tile_count hold no edges. `neg_ids`: entry j names a row of partition j // 8.
All inputs are finite; a program needn't handle non-finite values.
Results may differ from the reference program's by a relative error of at most 0.0012.
The reference program's roundings to bfloat16 on the way count: a program that leaves them out, or rounds other values in their place, can miss the bound.
Values may be sent and summed in bfloat16 or wider, within the bound.
A program may use at most 64 MiB of HBM per device.

```python
import jax
import jax.numpy as jnp
from jax import lax

H = 512
RELS = 2
FAN = 8
TILE = 256
NODE_DEV = 512
HALO_PEER = 4
MAX_TILES = 16
NEG_DEV = 8
NODES = 16384
NEG = 256
SLOTS = 640
N_DOM = 32


def draw_tile_count(key, part):
    first = jax.random.randint(jax.random.fold_in(key, 11), (N_DOM,), 0, MAX_TILES)
    second = jax.random.randint(jax.random.fold_in(key, 12), (N_DOM,), 0, MAX_TILES)
    counts = 1 + first * second // (2 * MAX_TILES)
    return jnp.where(jnp.arange(N_DOM) == N_DOM - 1, MAX_TILES, counts).astype(jnp.int32)


def touch_ends(values, own_key, low, top_value):
    longest = values.shape.index(max(values.shape))
    spots = []
    for shift in (0, 1):
        where = [jax.random.randint(jax.random.fold_in(own_key, axis), (), 0, length) for axis, length in enumerate(values.shape)]
        where[longest] = (where[longest] + shift) % values.shape[longest]
        spots.append(tuple(where))
    return values.at[spots[0]].set(low).at[spots[1]].set(top_value)


def levels(key, dims, split, low, largest):
    def one(axis_at, blocks):
        steps = jax.random.uniform(jax.random.fold_in(jax.random.fold_in(key, 6), axis_at), (blocks,), jnp.float32, low / len(split), largest / len(split))
        return jnp.repeat(jnp.exp(steps), dims[axis_at] // blocks).reshape((-1,) + (1,) * (len(dims) - axis_at - 1))

    factor_of = one(*split[0])
    for cut in split[1:]:
        factor_of = factor_of * one(*cut)
    return factor_of


def centred(key, extent, scale, limit, split=(), kind=jnp.bfloat16):
    entries = jax.random.normal(key, extent, jnp.float32) * scale
    if len(split) > 0:
        entries = levels(key, extent, split, -0.22, 0.18) * entries
    return jnp.clip(entries, min=-limit, max=limit).astype(kind)


def setup_inputs(seed: int = 0) -> dict:
    seeds = jax.random.split(jax.random.key(seed), 8)
    return {
        "features": centred(seeds[0], (NODES, H), 1.0, 6.0, ((0, 32),)),
        "weights": centred(seeds[1], (RELS + 1, H, H), (12 * H) ** -0.5, 0.078125),
        "halo_send": touch_ends(jax.random.randint(seeds[2], (N_DOM, N_DOM, HALO_PEER), 0, NODE_DEV), jax.random.fold_in(seeds[2], 1), 0, NODE_DEV - 1).astype(jnp.int32),
        "nbr_index": touch_ends(jax.random.randint(seeds[3], (NODES, RELS, FAN), 0, SLOTS), jax.random.fold_in(seeds[3], 1), 0, SLOTS - 1).astype(jnp.int32),
        "tile_count": draw_tile_count(jax.random.fold_in(seeds[7], 71), 0),
        "edge_ends": touch_ends(jax.random.randint(seeds[5], (N_DOM * MAX_TILES, 2, TILE), 0, NODE_DEV), jax.random.fold_in(seeds[5], 1), 0, NODE_DEV - 1).astype(jnp.int32),
        "neg_ids": touch_ends(jax.random.randint(seeds[6], (NEG,), 0, NODE_DEV), jax.random.fold_in(seeds[6], 1), 0, NODE_DEV - 1).astype(jnp.int32),
    }


def neighbour_mean(lookup, neighbours):
    running_sum = jnp.zeros((neighbours.shape[0], lookup.shape[1]), jnp.float32)
    for column in range(neighbours.shape[1]):
        running_sum = running_sum + lookup[neighbours[:, column]].astype(jnp.float32)
    return (running_sum / neighbours.shape[1]).astype(jnp.bfloat16)


def score_tile(source, target, negatives):
    source_wide = source.astype(jnp.float32)
    target_wide = target.astype(jnp.float32)
    positive = jnp.sum(source_wide * target_wide, axis=1)
    negative = lax.dot_general(source, negatives, (((1,), (1,)), ((), ())), preferred_element_type=jnp.float32)
    count_neg = negatives.shape[0]
    tile_loss = jnp.sum(jnp.logaddexp(0.0, -positive)) + jnp.sum(jnp.logaddexp(0.0, negative)) / count_neg
    grad_positive = -jax.nn.sigmoid(-positive)
    grad_negative = (jax.nn.sigmoid(negative) / count_neg).astype(jnp.bfloat16)
    source_grad = grad_positive[:, None] * target_wide + jnp.dot(grad_negative, negatives, preferred_element_type=jnp.float32)
    target_grad = grad_positive[:, None] * source_wide
    negative_grad = lax.dot_general(grad_negative, source, (((0,), (0,)), ((), ())), preferred_element_type=jnp.float32)
    return tile_loss, source_grad, target_grad, negative_grad


def reference(features, weights, halo_send, nbr_index, tile_count, edge_ends, neg_ids):
    def layer_part(partition):
        own_rows = lax.dynamic_slice_in_dim(features, partition * NODE_DEV, NODE_DEV, 0)
        sender = jnp.arange(N_DOM, dtype=jnp.int32)[:, None] * NODE_DEV
        halo_index = (sender + halo_send[:, partition, :]).reshape(-1).astype(jnp.int32)
        lookup = jnp.concatenate([own_rows, features[halo_index]], 0)
        neighbours = lax.dynamic_slice_in_dim(nbr_index, partition * NODE_DEV, NODE_DEV, 0)
        preact = jnp.dot(own_rows, weights[0], preferred_element_type=jnp.float32)
        means = []
        for relation in range(RELS):
            mean_rows = neighbour_mean(lookup, neighbours[:, relation, :])
            means.append(mean_rows)
            preact = preact + jnp.dot(mean_rows, weights[relation + 1], preferred_element_type=jnp.float32)
        return preact, jnp.stack(means)

    parts = jnp.arange(N_DOM, dtype=jnp.int32)
    preact, means = lax.map(layer_part, parts)
    embedding = preact.astype(jnp.bfloat16)
    flat_rows = embedding.reshape(-1, H)
    neg_rows = (jnp.arange(NEG, dtype=jnp.int32) // NEG_DEV) * NODE_DEV + neg_ids
    negatives = flat_rows[neg_rows]

    def per_part(state_now, partition):
        loss_sum, negative_total = state_now
        own_embed = embedding[partition]
        tile_ends = lax.dynamic_slice_in_dim(edge_ends, partition * MAX_TILES, MAX_TILES, 0)

        def tile_step(tile_index, running):
            tile_loss_sum, node_grad, neg_grad = running
            pair_ends = lax.dynamic_index_in_dim(tile_ends, tile_index, 0, keepdims=False)
            tile_loss, source_grad, target_grad, negative_grad = score_tile(own_embed[pair_ends[0]], own_embed[pair_ends[1]], negatives)
            node_grad = node_grad.at[pair_ends[0]].add(source_grad).at[pair_ends[1]].add(target_grad)
            return tile_loss_sum + tile_loss, node_grad, neg_grad + negative_grad

        initial = (jnp.zeros((), jnp.float32), jnp.zeros((NODE_DEV, H), jnp.float32), negative_total)
        tile_loss_sum, node_grad, negative_total = lax.fori_loop(0, tile_count[partition], tile_step, initial)
        return (loss_sum + tile_loss_sum, negative_total), node_grad

    start_state = (jnp.zeros((), jnp.float32), jnp.zeros((NEG, H), jnp.float32))
    (loss_sum, negative_total), node_grad = lax.scan(per_part, start_state, parts)
    node_grad = node_grad.reshape(-1, H).at[neg_rows].add(negative_total).reshape(N_DOM, NODE_DEV, H)
    pre_grad = node_grad.astype(jnp.bfloat16)
    feature_parts = features.reshape(N_DOM, NODE_DEV, H)

    def grad_part(running, items):
        own_rows, mean_rows, grad_rows = items
        terms = [lax.dot_general(own_rows, grad_rows, (((0,), (0,)), ((), ())), preferred_element_type=jnp.float32)]
        for relation in range(RELS):
            terms.append(lax.dot_general(mean_rows[relation], grad_rows, (((0,), (0,)), ((), ())), preferred_element_type=jnp.float32))
        return running + jnp.stack(terms), None

    weight_sum, unused = lax.scan(grad_part, jnp.zeros((RELS + 1, H, H), jnp.float32), (feature_parts, means, pre_grad))
    edge_total = jnp.sum(tile_count).astype(jnp.float32) * TILE
    return weight_sum / edge_total, loss_sum / edge_total, pre_grad.reshape(-1, H)
```

```python
import functools

import jax
import jax.numpy as jnp
from jax import lax
from jax.experimental import pallas as pl
from jax.experimental.pallas import tpu as pltpu
from jax.sharding import PartitionSpec as P

F32 = jnp.float32
BF16 = jnp.bfloat16
VMEM_LIMIT = 48 * 1024 * 1024


def whole(count):
    return [pl.BlockSpec(memory_space=pltpu.VMEM)] * count


def nn(a, b):
    return jnp.dot(a, b, preferred_element_type=F32)


def nt(a, b):
    return lax.dot_general(a, b, (((1,), (1,)), ((), ())), preferred_element_type=F32)


def tn(a, b):
    return lax.dot_general(a, b, (((0,), (0,)), ((), ())), preferred_element_type=F32)


def halves(x):
    high = x.astype(BF16)
    return high, (x - high.astype(F32)).astype(BF16)


def one_hot(mask):
    return jnp.where(mask, 1.0, 0.0).astype(BF16)


def prepare_kernel(fan, nbr_ref, ends_ref, count_ref, table_ref, pairs_ref, degree_ref):
    nodes, slots = table_ref.shape[1:]
    step = 64

    @pl.loop(0, nodes // step)
    def _(block):
        rows = pl.ds(pl.multiple_of(block * step, step), step)
        lanes = lax.broadcasted_iota(jnp.int32, (step, slots), 1)
        named = nbr_ref[rows, :]
        for relation in range(table_ref.shape[0]):
            total = jnp.zeros((step, slots), F32)
            for k in range(fan):
                column = relation * fan + k
                total = total + jnp.where(named[:, column : column + 1] == lanes, 1.0, 0.0)
            table_ref[relation, rows, :] = total.astype(BF16)

    pairs_ref[...] = jnp.zeros_like(pairs_ref)

    @pl.loop(0, count_ref[0])
    def _(tile):
        ends = ends_ref[tile]
        rows = lax.broadcasted_iota(jnp.int32, (nodes, ends.shape[1]), 0)
        pairs_ref[...] += nt(one_hot(ends[0:1, :] == rows), one_hot(ends[1:2, :] == rows))

    pairs = pairs_ref[...]
    degree_ref[...] = jnp.sum(pairs, axis=1, keepdims=True)
    pairs_ref[...] = pairs + pairs.T


def layer_kernel(fan, own_ref, halo_ref, weights_ref, table_ref, ids_ref, means_ref, embed_ref, neg_ref):
    nodes = own_ref.shape[0]
    own = own_ref[...]
    preact = nn(own, weights_ref[0])
    for relation in range(table_ref.shape[0]):
        total = nn(table_ref[relation, :, :nodes], own) + nn(table_ref[relation, :, nodes:], halo_ref[...])
        mean = (total / fan).astype(BF16)
        means_ref[relation] = mean
        preact = preact + nn(mean, weights_ref[relation + 1])
    embedding = preact.astype(BF16)
    embed_ref[...] = embedding
    lanes = lax.broadcasted_iota(jnp.int32, (ids_ref.shape[0], nodes), 1)
    neg_ref[...] = nn(one_hot(ids_ref[...] == lanes), embedding).astype(BF16)


def positive_kernel(embed_ref, pairs_ref, grad_ref, loss_ref):
    embedding = embed_ref[...]
    pairs = pairs_ref[...]
    score = nt(embedding, embedding)
    small = jnp.exp(-jnp.abs(score))
    loss = jnp.maximum(-score, 0.0) + jnp.log1p(small)
    loss_ref[...] = 0.5 * jnp.sum(pairs * loss, axis=0, keepdims=True)
    high, low = halves(-pairs * (jnp.where(score >= 0, small, 1.0) / (1.0 + small)))
    grad_ref[...] = nn(high, embedding) + nn(low, embedding)


def negative_kernel(embed_ref, negs_ref, degree_ref, positive_ref, grad_ref, neg_grad_ref, loss_ref):
    embedding = embed_ref[...]
    negatives = negs_ref[...]
    degree = degree_ref[...]
    count = negatives.shape[0]
    score = nt(embedding, negatives)
    small = jnp.exp(-jnp.abs(score))
    loss = jnp.maximum(score, 0.0) + jnp.log1p(small)
    loss_ref[...] = jnp.sum(degree * loss, axis=0, keepdims=True) / count
    slope = ((jnp.where(score >= 0, 1.0, small) / (1.0 + small)) / count).astype(BF16)
    grad_ref[...] = positive_ref[...] + degree * nn(slope, negatives)
    high, low = halves(degree * embedding.astype(F32))
    neg_grad_ref[...] = tn(slope, high) + tn(slope, low)


def gradient_kernel(own_ref, means_ref, grad_ref, neg_parts_ref, ids_ref, pre_ref, terms_ref):
    nodes = grad_ref.shape[0]
    total = neg_parts_ref[0]
    for part in range(1, neg_parts_ref.shape[0]):
        total = total + neg_parts_ref[part]
    rows = lax.broadcasted_iota(jnp.int32, (nodes, 1), 0)
    grad = grad_ref[...]
    for j in range(total.shape[0]):
        grad = grad + jnp.where(ids_ref[j : j + 1, :] == rows, total[j : j + 1, :], 0.0)
    pre = grad.astype(BF16)
    pre_ref[...] = pre
    terms_ref[0] = tn(own_ref[...], pre)
    for relation in range(means_ref.shape[0]):
        terms_ref[relation + 1] = tn(means_ref[relation], pre)


def call(kernel, out_shape, in_specs, **kwargs):
    many = isinstance(out_shape, (list, tuple))
    return pl.pallas_call(
        kernel,
        out_shape=out_shape,
        in_specs=in_specs,
        out_specs=whole(len(out_shape)) if many else whole(1)[0],
        compiler_params=pltpu.CompilerParams(vmem_limit_bytes=VMEM_LIMIT),
        **kwargs,
    )


def shape(dims, kind):
    return jax.ShapeDtypeStruct(dims, kind)


def on_device(parts, features, weights, halo_send, nbr_index, tile_count, edge_ends, neg_ids):
    nodes, width = features.shape
    relations, fan = nbr_index.shape[1:]
    per_peer = halo_send.shape[2]
    slots = nodes + parts * per_peer
    own_neg = neg_ids.shape[0]
    count_neg = own_neg * parts
    wanted = halo_send.reshape(-1, 1)
    columns = lax.broadcasted_iota(jnp.int32, (parts * per_peer, nodes), 1)
    outgoing = nn((wanted == columns).astype(BF16), features).astype(BF16)
    incoming = lax.all_to_all(
        outgoing.reshape(parts, per_peer, width), "dom", split_axis=0, concat_axis=0, tiled=True
    ).reshape(-1, width)
    table, pairs, degree = call(
        functools.partial(prepare_kernel, fan),
        (
            shape((relations, nodes, slots), BF16),
            shape((nodes, nodes), F32),
            shape((nodes, 1), F32),
        ),
        whole(2) + [pl.BlockSpec(memory_space=pltpu.SMEM)],
    )(nbr_index.reshape(nodes, relations * fan), edge_ends, tile_count)
    ids = neg_ids.reshape(-1, 1)
    means, embedding, my_negs = call(
        functools.partial(layer_kernel, fan),
        (
            shape((relations, nodes, width), BF16),
            shape((nodes, width), BF16),
            shape((own_neg, width), BF16),
        ),
        whole(5),
    )(features, incoming, weights, table, ids)
    negatives = lax.all_to_all(
        jnp.broadcast_to(my_negs[None], (parts, own_neg, width)), "dom", split_axis=0, concat_axis=0, tiled=True
    ).reshape(count_neg, width)
    positive_grad, loss_a = call(
        positive_kernel, (shape((nodes, width), F32), shape((1, nodes), F32)), whole(2)
    )(embedding, pairs)
    node_grad, neg_grad, loss_b = call(
        negative_kernel,
        (shape((nodes, width), F32), shape((count_neg, width), F32), shape((1, count_neg), F32)),
        whole(4),
    )(embedding, negatives, degree, positive_grad)
    neg_parts = lax.all_to_all(
        neg_grad.reshape(parts, own_neg, width), "dom", split_axis=0, concat_axis=0, tiled=True
    )
    pre_grad, terms = call(
        gradient_kernel,
        (shape((nodes, width), BF16), shape((relations + 1, width, width), F32)),
        whole(5),
    )(features, means, node_grad, neg_parts, ids)
    loss = jnp.sum(loss_a) + jnp.sum(loss_b)
    edges = tile_count[0].astype(F32) * edge_ends.shape[2]
    weight_sum, total_loss, edge_total = lax.psum((terms, loss, edges), "dom")
    return (weight_sum / edge_total, total_loss / edge_total, pre_grad)


def solution(mesh):
    placed = (
        P("dom", None),
        P(),
        P("dom", None, None),
        P("dom", None, None),
        P("dom"),
        P("dom", None, None),
        P("dom"),
    )
    return jax.shard_map(
        functools.partial(on_device, mesh.shape["dom"]),
        mesh=mesh,
        in_specs=placed,
        out_specs=(P(), P(), P("dom", None)),
        check_vma=False,
    )
```

```python
import functools

import jax
import jax.numpy as jnp
from jax import lax
from jax.experimental import pallas as pl
from jax.experimental.pallas import tpu as pltpu
from jax.sharding import PartitionSpec as P

F32 = jnp.float32
BF16 = jnp.bfloat16
VMEM_LIMIT = 48 * 1024 * 1024
LANES = 128
MESH = pl.DeviceIdType.MESH


def whole(count):
    return [pl.BlockSpec(memory_space=pltpu.VMEM)] * count


def nn(a, b):
    return jnp.dot(a, b, preferred_element_type=F32)


def nt(a, b):
    return lax.dot_general(a, b, (((1,), (1,)), ((), ())), preferred_element_type=F32)


def tn(a, b):
    return lax.dot_general(a, b, (((0,), (0,)), ((), ())), preferred_element_type=F32)


def halves(x):
    high = x.astype(BF16)
    return high, (x - high.astype(F32)).astype(BF16)


def one_hot(mask):
    return jnp.where(mask, 1.0, 0.0).astype(BF16)


def prepare_kernel(fan, nbr_ref, ends_ref, count_ref, table_ref, pairs_ref, degree_ref):
    nodes, slots = table_ref.shape[1:]
    step = 64

    @pl.loop(0, nodes // step)
    def _(block):
        rows = pl.ds(pl.multiple_of(block * step, step), step)
        lanes = lax.broadcasted_iota(jnp.int32, (step, slots), 1)
        named = nbr_ref[rows, :]
        for relation in range(table_ref.shape[0]):
            total = jnp.zeros((step, slots), F32)
            for k in range(fan):
                column = relation * fan + k
                total = total + jnp.where(named[:, column : column + 1] == lanes, 1.0, 0.0)
            table_ref[relation, rows, :] = total.astype(BF16)

    pairs_ref[...] = jnp.zeros_like(pairs_ref)

    @pl.loop(0, count_ref[0])
    def _(tile):
        ends = ends_ref[tile]
        rows = lax.broadcasted_iota(jnp.int32, (nodes, ends.shape[1]), 0)
        pairs_ref[...] += nt(one_hot(ends[0:1, :] == rows), one_hot(ends[1:2, :] == rows))

    pairs = pairs_ref[...]
    degree_ref[...] = jnp.sum(pairs, axis=1, keepdims=True)
    pairs_ref[...] = pairs + pairs.T


def layer_kernel(fan, own_ref, halo_ref, weights_ref, table_ref, ids_ref, means_ref, embed_ref, neg_ref):
    nodes = own_ref.shape[0]
    own = own_ref[...]
    preact = nn(own, weights_ref[0])
    for relation in range(table_ref.shape[0]):
        total = nn(table_ref[relation, :, :nodes], own) + nn(table_ref[relation, :, nodes:], halo_ref[...])
        mean = (total / fan).astype(BF16)
        means_ref[relation] = mean
        preact = preact + nn(mean, weights_ref[relation + 1])
    embedding = preact.astype(BF16)
    embed_ref[...] = embedding
    lanes = lax.broadcasted_iota(jnp.int32, (ids_ref.shape[0], nodes), 1)
    neg_ref[...] = nn(one_hot(ids_ref[...] == lanes), embedding).astype(BF16)


def positive_kernel(embed_ref, pairs_ref, grad_ref, loss_ref):
    embedding = embed_ref[...]
    pairs = pairs_ref[...]
    score = nt(embedding, embedding)
    small = jnp.exp(-jnp.abs(score))
    loss = jnp.maximum(-score, 0.0) + jnp.log1p(small)
    loss_ref[...] = 0.5 * jnp.sum(pairs * loss, axis=0, keepdims=True)
    high, low = halves(-pairs * (jnp.where(score >= 0, small, 1.0) / (1.0 + small)))
    grad_ref[...] = nn(high, embedding) + nn(low, embedding)


def negative_kernel(embed_ref, negs_ref, degree_ref, positive_ref, loss_ref, count_ref, edge_ref, grad_ref, send_ref):
    parts, own_neg, _ = send_ref.shape
    embedding = embed_ref[...]
    width = embedding.shape[1]
    negatives = negs_ref[...]
    degree = degree_ref[...]
    count = negatives.shape[0]
    score = nt(embedding, negatives)
    small = jnp.exp(-jnp.abs(score))
    loss = jnp.maximum(score, 0.0) + jnp.log1p(small)
    loss_sum = jnp.sum(loss_ref[...]) + jnp.sum(degree * loss) / count
    slope = ((jnp.where(score >= 0, 1.0, small) / (1.0 + small)) / count).astype(BF16)
    grad_ref[...] = positive_ref[...] + degree * nn(slope, negatives)
    high, low = halves(degree * embedding.astype(F32))
    neg_grad = tn(slope, high) + tn(slope, low)
    send_ref[:, :, :width] = neg_grad.reshape(parts, own_neg, width)
    edges = count_ref[0].astype(F32) * edge_ref.shape[1]
    rows = lax.broadcasted_iota(jnp.int32, (own_neg, LANES), 0)
    tile = jnp.where(rows == 0, loss_sum, edges)
    send_ref[:, :, width:] = jnp.broadcast_to(tile[None], (parts, own_neg, LANES))


def greet(peers):
    barrier = pltpu.get_barrier_semaphore()
    for peer in peers:
        pl.semaphore_signal(barrier, inc=1, device_id=(peer,), device_id_type=MESH)
    pl.semaphore_wait(barrier, len(peers))


def exchange_kernel(parts, send_ref, total_ref, landed, send_sem, recv_sem):
    me = lax.axis_index("dom")
    barrier = pltpu.get_barrier_semaphore()

    def copy_to(peer, slot, sem):
        return pltpu.make_async_remote_copy(
            src_ref=send_ref.at[peer],
            dst_ref=landed.at[slot],
            send_sem=send_sem.at[sem],
            recv_sem=recv_sem.at[slot],
            device_id=(peer,),
            device_id_type=MESH,
        )

    @pl.loop(1, parts)
    def _(i):
        pl.semaphore_signal(barrier, inc=1, device_id=((me + i) % parts,), device_id_type=MESH)

    pl.semaphore_wait(barrier, parts - 1)

    @pl.loop(1, parts)
    def _(i):
        copy_to((me + i) % parts, me, i).start()

    landed[me] = send_ref[me]

    @pl.loop(1, parts)
    def _(i):
        copy_to((me + i) % parts, (me + i) % parts, i).wait()

    total = landed[0]
    for part in range(1, parts):
        total = total + landed[part]
    total_ref[...] = total


def reduce_plan(parts, colors):
    radix = [1, 1, 1]
    at = 0
    while radix[0] * radix[1] * radix[2] * 2 < parts:
        radix[at % 3] *= 2
        at += 1
    outer, middle, inner = radix
    core = (2, 1)
    dims = [(inner, 2), (middle, 2 * inner), (outer, 2 * inner * middle)]
    return [[core] + [dims[(color + k) % 3] for k in range(3)] for color in range(colors)]


def reduce_kernel(plan, terms_ref, edges_ref, out_ref, *scratch):
    colors = len(plan)
    phases = len(plan[0])
    me = lax.axis_index("dom")
    landed = [scratch[color * phases : (color + 1) * phases] for color in range(colors)]
    scratch = scratch[colors * phases :]
    sums = [scratch[color * phases : (color + 1) * phases] for color in range(colors)]
    send_sem, recv_sem = scratch[colors * phases :]
    spots = {}

    def spot(*key):
        return spots.setdefault(key, len(spots))

    def place(color, phase):
        size, stride = plan[color][phase]
        return size, stride, (me // stride) % size

    def remote(source, target, key, peer):
        at = spot(*key)
        return pltpu.make_async_remote_copy(
            src_ref=source,
            dst_ref=target,
            send_sem=send_sem.at[at],
            recv_sem=recv_sem.at[at],
            device_id=(peer,),
            device_id_type=MESH,
        )

    greet([
        me + ((me // stride + delta) % size - (me // stride) % size) * stride
        for size, stride in plan[0]
        for delta in range(1, size)
    ])

    def scatter_copies(color, phase):
        size, stride, mine = place(color, phase)
        source = terms_ref.at[color] if phase == 0 else sums[color][phase - 1]
        length = source.shape[0] // size
        copies = []
        for delta in range(1, size):
            other = (mine + delta) % size
            copies.append(
                remote(
                    source.at[pl.ds(other * length, length)],
                    landed[color][phase].at[delta - 1],
                    ("scatter", color, phase, delta),
                    me + (other - mine) * stride,
                )
            )
        return copies

    def regions(color):
        off, length = 0, terms_ref.shape[1]
        found = [(off, length)]
        for phase in range(phases):
            size, _, mine = place(color, phase)
            length = length // size
            off = off + mine * length
            found.append((off, length))
        return found

    def gather_copies(color, phase):
        size, stride, mine = place(color, phase)
        off, length = regions(color)[phase + 1]
        block = out_ref.at[color, pl.ds(off, length)]
        return [
            remote(block, block, ("gather", color, phase, delta), me + ((mine + delta) % size - mine) * stride)
            for delta in range(1, size)
        ]

    flying = [scatter_copies(color, 0) for color in range(colors)]
    for copies in flying:
        for copy in copies:
            copy.start()
    for phase in range(phases):
        for color in range(colors):
            for copy in flying[color]:
                copy.wait()
            size, _, mine = place(color, phase)
            source = terms_ref.at[color] if phase == 0 else sums[color][phase - 1]
            length = source.shape[0] // size
            total = source[pl.ds(mine * length, length)]
            for slot in range(size - 1):
                total = total + landed[color][phase][slot]
            if phase < phases - 1:
                sums[color][phase][...] = total
                flying[color] = scatter_copies(color, phase + 1)
            else:
                off, length = regions(color)[phases]
                out_ref[color, pl.ds(off, length)] = total / edges_ref[...][None]
                flying[color] = gather_copies(color, phase)
            for copy in flying[color]:
                copy.start()
    for phase in reversed(range(phases)):
        for color in range(colors):
            for copy in flying[color]:
                copy.wait()
            if phase > 0:
                flying[color] = gather_copies(color, phase - 1)
                for copy in flying[color]:
                    copy.start()


def gradient_kernel(own_ref, means_ref, grad_ref, total_ref, ids_ref, pre_ref, terms_ref, edges_ref, loss_ref):
    nodes, width = grad_ref.shape
    total = total_ref[...]
    rows = lax.broadcasted_iota(jnp.int32, (nodes, 1), 0)
    grad = grad_ref[...]
    for j in range(total.shape[0]):
        grad = grad + jnp.where(ids_ref[j : j + 1, :] == rows, total[j : j + 1, :width], 0.0)
    pre = grad.astype(BF16)
    pre_ref[...] = pre
    tall = width // 8
    for term in range(terms_ref.shape[0]):
        left = own_ref[...] if term == 0 else means_ref[term - 1]
        product = tn(left, pre)
        for j in range(width // LANES):
            terms_ref[term, j * tall : (j + 1) * tall] = product[:, j * LANES : (j + 1) * LANES].reshape(tall, 8, LANES)
    edges = total[1:2, width:]
    edges_ref[...] = jnp.broadcast_to(edges, edges_ref.shape)
    loss_ref[...] = total[0:1, width:] / edges


def finish_kernel(tiles_ref, out_ref):
    width = out_ref.shape[2]
    tall = width // 8
    for term in range(out_ref.shape[0]):
        for j in range(width // LANES):
            out_ref[term, :, j * LANES : (j + 1) * LANES] = tiles_ref[term, j * tall : (j + 1) * tall].reshape(width, LANES)


def call(kernel, out_shape, in_specs, collective=None, **kwargs):
    extra = {} if collective is None else {"collective_id": collective, "has_side_effects": True}
    many = isinstance(out_shape, (list, tuple))
    return pl.pallas_call(
        kernel,
        out_shape=out_shape,
        in_specs=in_specs,
        out_specs=whole(len(out_shape)) if many else whole(1)[0],
        compiler_params=pltpu.CompilerParams(vmem_limit_bytes=VMEM_LIMIT, **extra),
        **kwargs,
    )


def shape(dims, kind):
    return jax.ShapeDtypeStruct(dims, kind)


def on_device(parts, features, weights, halo_send, nbr_index, tile_count, edge_ends, neg_ids):
    nodes, width = features.shape
    relations, fan = nbr_index.shape[1:]
    per_peer = halo_send.shape[2]
    slots = nodes + parts * per_peer
    own_neg = neg_ids.shape[0]
    count_neg = own_neg * parts
    wanted = halo_send.reshape(-1, 1)
    columns = lax.broadcasted_iota(jnp.int32, (parts * per_peer, nodes), 1)
    outgoing = nn((wanted == columns).astype(BF16), features).astype(BF16)
    incoming = lax.all_to_all(
        outgoing.reshape(parts, per_peer, width), "dom", split_axis=0, concat_axis=0, tiled=True
    ).reshape(-1, width)
    table, pairs, degree = call(
        functools.partial(prepare_kernel, fan),
        (
            shape((relations, nodes, slots), BF16),
            shape((nodes, nodes), F32),
            shape((nodes, 1), F32),
        ),
        whole(2) + [pl.BlockSpec(memory_space=pltpu.SMEM)],
    )(nbr_index.reshape(nodes, relations * fan), edge_ends, tile_count)
    ids = neg_ids.reshape(-1, 1)
    means, embedding, my_negs = call(
        functools.partial(layer_kernel, fan),
        (
            shape((relations, nodes, width), BF16),
            shape((nodes, width), BF16),
            shape((own_neg, width), BF16),
        ),
        whole(5),
    )(features, incoming, weights, table, ids)
    negatives = lax.all_to_all(
        jnp.broadcast_to(my_negs[None], (parts, own_neg, width)), "dom", split_axis=0, concat_axis=0, tiled=True
    ).reshape(count_neg, width)
    positive_grad, loss_a = call(
        positive_kernel, (shape((nodes, width), F32), shape((1, nodes), F32)), whole(2)
    )(embedding, pairs)
    node_grad, outbound = call(
        negative_kernel,
        (shape((nodes, width), F32), shape((parts, own_neg, width + LANES), F32)),
        whole(5) + [pl.BlockSpec(memory_space=pltpu.SMEM), pl.BlockSpec(memory_space=pltpu.VMEM)],
    )(embedding, negatives, degree, positive_grad, loss_a, tile_count, edge_ends[0])
    total = call(
        functools.partial(exchange_kernel, parts),
        shape((own_neg, width + LANES), F32),
        whole(1),
        collective=1,
        scratch_shapes=[
            pltpu.VMEM(outbound.shape, F32),
            pltpu.SemaphoreType.DMA((parts,)),
            pltpu.SemaphoreType.DMA((parts,)),
        ],
    )(outbound)
    tiles = (relations + 1, width * width // (8 * LANES), 8, LANES)
    pre_grad, terms, edges, loss = call(
        gradient_kernel,
        (shape((nodes, width), BF16), shape(tiles, F32), shape((8, LANES), F32), shape((1, LANES), F32)),
        whole(5),
    )(features, means, node_grad, total, ids)
    plan = reduce_plan(parts, tiles[0])
    landed, sums, copies = [], [], 0
    for dims in plan:
        length = tiles[1]
        for size, _ in dims:
            length = length // size
            landed.append(pltpu.VMEM((size - 1, length, 8, LANES), F32))
            sums.append(pltpu.VMEM((length, 8, LANES), F32))
            copies += 2 * (size - 1)
    reduced = call(
        functools.partial(reduce_kernel, plan),
        shape(tiles, F32),
        whole(2),
        collective=2,
        scratch_shapes=landed + sums + [pltpu.SemaphoreType.DMA((copies,)), pltpu.SemaphoreType.DMA((copies,))],
    )(terms, edges)
    weight_grad = call(finish_kernel, shape((relations + 1, width, width), F32), whole(1))(reduced)
    return (weight_grad, loss[0, 0], pre_grad)


def solution(mesh):
    placed = (
        P("dom", None),
        P(),
        P("dom", None, None),
        P("dom", None, None),
        P("dom"),
        P("dom", None, None),
        P("dom"),
    )
    return jax.shard_map(
        functools.partial(on_device, mesh.shape["dom"]),
        mesh=mesh,
        in_specs=placed,
        out_specs=(P(), P(), P("dom", None)),
        check_vma=False,
    )
```

```python
import functools

import jax
import jax.numpy as jnp
from jax import lax
from jax.experimental import pallas as pl
from jax.experimental.pallas import tpu as pltpu
from jax.sharding import PartitionSpec as P

F32 = jnp.float32
BF16 = jnp.bfloat16
VMEM_LIMIT = 48 * 1024 * 1024
LANES = 128
MESH = pl.DeviceIdType.MESH


def whole(count):
    return [pl.BlockSpec(memory_space=pltpu.VMEM)] * count


def nn(a, b):
    return jnp.dot(a, b, preferred_element_type=F32)


def nt(a, b):
    return lax.dot_general(a, b, (((1,), (1,)), ((), ())), preferred_element_type=F32)


def tn(a, b):
    return lax.dot_general(a, b, (((0,), (0,)), ((), ())), preferred_element_type=F32)


def halves(x):
    high = x.astype(BF16)
    return high, (x - high.astype(F32)).astype(BF16)


def one_hot(mask):
    return jnp.where(mask, 1.0, 0.0).astype(BF16)


def prepare_kernel(fan, nbr_ref, ends_ref, count_ref, table_ref, pairs_ref, degree_ref):
    nodes, slots = table_ref.shape[1:]
    step = 64

    @pl.loop(0, nodes // step)
    def _(block):
        rows = pl.ds(pl.multiple_of(block * step, step), step)
        lanes = lax.broadcasted_iota(jnp.int32, (step, slots), 1)
        named = nbr_ref[rows, :]
        for relation in range(table_ref.shape[0]):
            total = jnp.zeros((step, slots), F32)
            for k in range(fan):
                column = relation * fan + k
                total = total + jnp.where(named[:, column : column + 1] == lanes, 1.0, 0.0)
            table_ref[relation, rows, :] = total.astype(BF16)

    pairs_ref[...] = jnp.zeros_like(pairs_ref)

    @pl.loop(0, count_ref[0])
    def _(tile):
        ends = ends_ref[tile]
        rows = lax.broadcasted_iota(jnp.int32, (nodes, ends.shape[1]), 0)
        pairs_ref[...] += nt(one_hot(ends[0:1, :] == rows), one_hot(ends[1:2, :] == rows))

    pairs = pairs_ref[...]
    degree_ref[...] = jnp.sum(pairs, axis=1, keepdims=True)
    pairs_ref[...] = pairs + pairs.T


def layer_kernel(fan, own_ref, halo_ref, weights_ref, table_ref, ids_ref, means_ref, embed_ref, neg_ref):
    nodes = own_ref.shape[0]
    own = own_ref[...]
    preact = nn(own, weights_ref[0])
    for relation in range(table_ref.shape[0]):
        total = nn(table_ref[relation, :, :nodes], own) + nn(table_ref[relation, :, nodes:], halo_ref[...])
        mean = (total / fan).astype(BF16)
        means_ref[relation] = mean
        preact = preact + nn(mean, weights_ref[relation + 1])
    embedding = preact.astype(BF16)
    embed_ref[...] = embedding
    lanes = lax.broadcasted_iota(jnp.int32, (ids_ref.shape[0], nodes), 1)
    neg_ref[...] = nn(one_hot(ids_ref[...] == lanes), embedding).astype(BF16)


def positive_kernel(embed_ref, pairs_ref, grad_ref, loss_ref):
    embedding = embed_ref[...]
    pairs = pairs_ref[...]
    score = nt(embedding, embedding)
    small = jnp.exp(-jnp.abs(score))
    loss = jnp.maximum(-score, 0.0) + jnp.log1p(small)
    loss_ref[...] = 0.5 * jnp.sum(pairs * loss, axis=0, keepdims=True)
    high, low = halves(-pairs * (jnp.where(score >= 0, small, 1.0) / (1.0 + small)))
    grad_ref[...] = nn(high, embedding) + nn(low, embedding)


def negative_kernel(embed_ref, negs_ref, degree_ref, positive_ref, loss_ref, count_ref, edge_ref, grad_ref, send_ref):
    _, chips, own_neg, _ = send_ref.shape
    embedding = embed_ref[...]
    width = embedding.shape[1]
    negatives = negs_ref[...]
    degree = degree_ref[...]
    count = negatives.shape[0]
    score = nt(embedding, negatives)
    small = jnp.exp(-jnp.abs(score))
    loss = jnp.maximum(score, 0.0) + jnp.log1p(small)
    loss_sum = jnp.sum(loss_ref[...]) + jnp.sum(degree * loss) / count
    slope = ((jnp.where(score >= 0, 1.0, small) / (1.0 + small)) / count).astype(BF16)
    grad_ref[...] = positive_ref[...] + degree * nn(slope, negatives)
    high, low = halves(degree * embedding.astype(F32))
    neg_grad = tn(slope, high) + tn(slope, low)
    blocks = neg_grad.reshape(chips, 2, own_neg, width)
    for core in range(2):
        send_ref[core, :, :, :width] = blocks[:, core]
    edges = count_ref[0].astype(F32) * edge_ref.shape[1]
    rows = lax.broadcasted_iota(jnp.int32, (own_neg, LANES), 0)
    tile = jnp.where(rows == 0, loss_sum, edges)
    send_ref[:, :, :, width:] = jnp.broadcast_to(tile[None, None], (2, chips, own_neg, LANES))


def greet(peers):
    barrier = pltpu.get_barrier_semaphore()
    for peer in peers:
        pl.semaphore_signal(barrier, inc=1, device_id=(peer,), device_id_type=MESH)
    pl.semaphore_wait(barrier, len(peers))


def exchange_kernel(parts, send_ref, total_ref, paired, chip, landed, pair_sem, send_sem, recv_sem):
    me = lax.axis_index("dom")
    core = me % 2
    place = me // 2
    chips = parts // 2
    barrier = pltpu.get_barrier_semaphore()
    partner = me + 1 - 2 * core

    def copy_to(other, slot, sem):
        return pltpu.make_async_remote_copy(
            src_ref=chip.at[other],
            dst_ref=landed.at[slot],
            send_sem=send_sem.at[sem],
            recv_sem=recv_sem.at[slot],
            device_id=(2 * other + core,),
            device_id_type=MESH,
        )

    pl.semaphore_signal(barrier, inc=1, device_id=(partner,), device_id_type=MESH)

    @pl.loop(1, chips)
    def _(i):
        pl.semaphore_signal(barrier, inc=1, device_id=(2 * ((place + i) % chips) + core,), device_id_type=MESH)

    pl.semaphore_wait(barrier, chips)
    pair = pltpu.make_async_remote_copy(
        src_ref=send_ref.at[1 - core],
        dst_ref=paired,
        send_sem=pair_sem.at[0],
        recv_sem=pair_sem.at[1],
        device_id=(partner,),
        device_id_type=MESH,
    )
    pair.start()
    pair.wait()
    chip[...] = send_ref[core] + paired[...]

    @pl.loop(1, chips)
    def _(i):
        copy_to((place + i) % chips, place, i).start()

    landed[place] = chip[place]

    @pl.loop(1, chips)
    def _(i):
        copy_to((place + i) % chips, (place + i) % chips, i).wait()

    total = landed[0]
    for other in range(1, chips):
        total = total + landed[other]
    total_ref[...] = total


def reduce_plan(parts, colors):
    radix = [1, 1, 1]
    at = 0
    while radix[0] * radix[1] * radix[2] * 2 < parts:
        radix[at % 3] *= 2
        at += 1
    outer, middle, inner = radix
    core, first, second, last = (2, 1), (inner, 2), (middle, 2 * inner), (outer, 2 * inner * middle)
    return [[core, first, second, last] if color % 2 == 0 else [core, second, first, last] for color in range(colors)]


def reduce_kernel(plan, terms_ref, edges_ref, out_ref, *scratch):
    colors = len(plan)
    phases = len(plan[0])
    me = lax.axis_index("dom")
    landed = [scratch[color * phases : (color + 1) * phases] for color in range(colors)]
    scratch = scratch[colors * phases :]
    sums = [scratch[color * phases : (color + 1) * phases] for color in range(colors)]
    send_sem, recv_sem = scratch[colors * phases :]
    spots = {}

    def spot(*key):
        return spots.setdefault(key, len(spots))

    def place(color, phase):
        size, stride = plan[color][phase]
        return size, stride, (me // stride) % size

    def remote(source, target, key, peer):
        at = spot(*key)
        return pltpu.make_async_remote_copy(
            src_ref=source,
            dst_ref=target,
            send_sem=send_sem.at[at],
            recv_sem=recv_sem.at[at],
            device_id=(peer,),
            device_id_type=MESH,
        )

    greet([
        me + ((me // stride + delta) % size - (me // stride) % size) * stride
        for size, stride in plan[0]
        for delta in range(1, size)
    ])

    def scatter_copies(color, phase):
        size, stride, mine = place(color, phase)
        source = terms_ref.at[color] if phase == 0 else sums[color][phase - 1]
        length = source.shape[0] // size
        copies = []
        for delta in range(1, size):
            other = (mine + delta) % size
            copies.append(
                remote(
                    source.at[pl.ds(other * length, length)],
                    landed[color][phase].at[delta - 1],
                    ("scatter", color, phase, delta),
                    me + (other - mine) * stride,
                )
            )
        return copies

    def regions(color):
        off, length = 0, terms_ref.shape[1]
        found = [(off, length)]
        for phase in range(phases):
            size, _, mine = place(color, phase)
            length = length // size
            off = off + mine * length
            found.append((off, length))
        return found

    def gather_copies(color, phase):
        size, stride, mine = place(color, phase)
        off, length = regions(color)[phase + 1]
        block = out_ref.at[color, pl.ds(off, length)]
        return [
            remote(block, block, ("gather", color, phase, delta), me + ((mine + delta) % size - mine) * stride)
            for delta in range(1, size)
        ]

    flying = [scatter_copies(color, 0) for color in range(colors)]
    for copies in flying:
        for copy in copies:
            copy.start()
    for phase in range(phases):
        for color in range(colors):
            for copy in flying[color]:
                copy.wait()
            size, _, mine = place(color, phase)
            source = terms_ref.at[color] if phase == 0 else sums[color][phase - 1]
            length = source.shape[0] // size
            total = source[pl.ds(mine * length, length)]
            for slot in range(size - 1):
                total = total + landed[color][phase][slot]
            if phase < phases - 1:
                sums[color][phase][...] = total
                flying[color] = scatter_copies(color, phase + 1)
            else:
                off, length = regions(color)[phases]
                out_ref[color, pl.ds(off, length)] = total / edges_ref[...][None]
                flying[color] = gather_copies(color, phase)
            for copy in flying[color]:
                copy.start()
    for phase in reversed(range(phases)):
        for color in range(colors):
            for copy in flying[color]:
                copy.wait()
            if phase > 0:
                flying[color] = gather_copies(color, phase - 1)
                for copy in flying[color]:
                    copy.start()


def gradient_kernel(own_ref, means_ref, grad_ref, total_ref, ids_ref, pre_ref, terms_ref, edges_ref, loss_ref):
    nodes, width = grad_ref.shape
    total = total_ref[...]
    rows = lax.broadcasted_iota(jnp.int32, (nodes, 1), 0)
    grad = grad_ref[...]
    for j in range(total.shape[0]):
        grad = grad + jnp.where(ids_ref[j : j + 1, :] == rows, total[j : j + 1, :width], 0.0)
    pre = grad.astype(BF16)
    pre_ref[...] = pre
    tall = width // 8
    for term in range(terms_ref.shape[0]):
        left = own_ref[...] if term == 0 else means_ref[term - 1]
        product = tn(left, pre)
        for j in range(width // LANES):
            terms_ref[term, j * tall : (j + 1) * tall] = product[:, j * LANES : (j + 1) * LANES].reshape(tall, 8, LANES)
    edges = total[1:2, width:]
    edges_ref[...] = jnp.broadcast_to(edges, edges_ref.shape)
    loss_ref[...] = total[0:1, width:] / edges


def finish_kernel(tiles_ref, out_ref):
    width = out_ref.shape[2]
    tall = width // 8
    for term in range(out_ref.shape[0]):
        for j in range(width // LANES):
            out_ref[term, :, j * LANES : (j + 1) * LANES] = tiles_ref[term, j * tall : (j + 1) * tall].reshape(width, LANES)


def call(kernel, out_shape, in_specs, collective=None, **kwargs):
    extra = {} if collective is None else {"collective_id": collective, "has_side_effects": True}
    many = isinstance(out_shape, (list, tuple))
    return pl.pallas_call(
        kernel,
        out_shape=out_shape,
        in_specs=in_specs,
        out_specs=whole(len(out_shape)) if many else whole(1)[0],
        compiler_params=pltpu.CompilerParams(vmem_limit_bytes=VMEM_LIMIT, **extra),
        **kwargs,
    )


def shape(dims, kind):
    return jax.ShapeDtypeStruct(dims, kind)


def on_device(parts, features, weights, halo_send, nbr_index, tile_count, edge_ends, neg_ids):
    nodes, width = features.shape
    relations, fan = nbr_index.shape[1:]
    per_peer = halo_send.shape[2]
    slots = nodes + parts * per_peer
    own_neg = neg_ids.shape[0]
    count_neg = own_neg * parts
    wanted = halo_send.reshape(-1, 1)
    columns = lax.broadcasted_iota(jnp.int32, (parts * per_peer, nodes), 1)
    outgoing = nn((wanted == columns).astype(BF16), features).astype(BF16)
    incoming = lax.all_to_all(
        outgoing.reshape(parts, per_peer, width), "dom", split_axis=0, concat_axis=0, tiled=True
    ).reshape(-1, width)
    table, pairs, degree = call(
        functools.partial(prepare_kernel, fan),
        (
            shape((relations, nodes, slots), BF16),
            shape((nodes, nodes), F32),
            shape((nodes, 1), F32),
        ),
        whole(2) + [pl.BlockSpec(memory_space=pltpu.SMEM)],
    )(nbr_index.reshape(nodes, relations * fan), edge_ends, tile_count)
    ids = neg_ids.reshape(-1, 1)
    means, embedding, my_negs = call(
        functools.partial(layer_kernel, fan),
        (
            shape((relations, nodes, width), BF16),
            shape((nodes, width), BF16),
            shape((own_neg, width), BF16),
        ),
        whole(5),
    )(features, incoming, weights, table, ids)
    negatives = lax.all_to_all(
        jnp.broadcast_to(my_negs[None], (parts, own_neg, width)), "dom", split_axis=0, concat_axis=0, tiled=True
    ).reshape(count_neg, width)
    positive_grad, loss_a = call(
        positive_kernel, (shape((nodes, width), F32), shape((1, nodes), F32)), whole(2)
    )(embedding, pairs)
    node_grad, outbound = call(
        negative_kernel,
        (shape((nodes, width), F32), shape((2, parts // 2, own_neg, width + LANES), F32)),
        whole(5) + [pl.BlockSpec(memory_space=pltpu.SMEM), pl.BlockSpec(memory_space=pltpu.VMEM)],
    )(embedding, negatives, degree, positive_grad, loss_a, tile_count, edge_ends[0])
    total = call(
        functools.partial(exchange_kernel, parts),
        shape((own_neg, width + LANES), F32),
        whole(1),
        collective=1,
        scratch_shapes=[
            pltpu.VMEM(outbound.shape[1:], F32),
            pltpu.VMEM(outbound.shape[1:], F32),
            pltpu.VMEM(outbound.shape[1:], F32),
            pltpu.SemaphoreType.DMA((2,)),
            pltpu.SemaphoreType.DMA((parts // 2,)),
            pltpu.SemaphoreType.DMA((parts // 2,)),
        ],
    )(outbound)
    tiles = (relations + 1, width * width // (8 * LANES), 8, LANES)
    pre_grad, terms, edges, loss = call(
        gradient_kernel,
        (shape((nodes, width), BF16), shape(tiles, F32), shape((8, LANES), F32), shape((1, LANES), F32)),
        whole(5),
    )(features, means, node_grad, total, ids)
    pieces = (2 * tiles[0], tiles[1] // 2, *tiles[2:])
    plan = reduce_plan(parts, pieces[0])
    landed, sums, copies = [], [], 0
    for dims in plan:
        length = pieces[1]
        for size, _ in dims:
            length = length // size
            landed.append(pltpu.VMEM((size - 1, length, 8, LANES), F32))
            sums.append(pltpu.VMEM((length, 8, LANES), F32))
            copies += 2 * (size - 1)
    reduced = call(
        functools.partial(reduce_kernel, plan),
        shape(pieces, F32),
        whole(2),
        collective=2,
        scratch_shapes=landed + sums + [pltpu.SemaphoreType.DMA((copies,)), pltpu.SemaphoreType.DMA((copies,))],
    )(terms.reshape(pieces), edges)
    weight_grad = call(finish_kernel, shape((relations + 1, width, width), F32), whole(1))(reduced.reshape(tiles))
    return (weight_grad, loss[0, 0], pre_grad)


def solution(mesh):
    placed = (
        P("dom", None),
        P(),
        P("dom", None, None),
        P("dom", None, None),
        P("dom"),
        P("dom", None, None),
        P("dom"),
    )
    return jax.shard_map(
        functools.partial(on_device, mesh.shape["dom"]),
        mesh=mesh,
        in_specs=placed,
        out_specs=(P(), P(), P("dom", None)),
        check_vma=False,
    )
```
